32 devices in a mesh: replica: 8 (over z, x), shard: 4 (over y, core).
Axes of the slice: x: 2, y: 2, z: 4, core: 2. Of those that a mesh axis runs over, the one named last changes fastest.
Arguments:
- activations: bfloat16 [8192, 1536], P('replica'), may hold values from -6 to 6
- output_grads: bfloat16 [8192, 4, 1536], P('replica', None, 'shard'), may hold values from -0.009765625 to 0.009765625
- owner: int32 [4], replicated, may hold values from 0 to 3, each once
- step_count: int32 [1], replicated, may hold values from 1 to 40
- statistics: float32 [6144, 2, 1536], P(('replica', 'shard')), may hold values from -6 to 6
- inverse_roots: bfloat16 [6144, 2, 1536], P(('replica', 'shard')), may hold values from -1 to 2, as said below
- first_moment: float32 [6144, 1536], P(('replica', 'shard')), may hold values from -0.6 to 0.6
- second_moment: float32 [6144, 1536], P(('replica', 'shard')), may hold values from 0.005 to 0.05
Outputs:
- new_statistics: float32 [6144, 2, 1536], P(('replica', 'shard'))
- new_first: float32 [6144, 1536], P(('replica', 'shard'))
- new_second: float32 [6144, 1536], P(('replica', 'shard'))
- update: bfloat16 [4, 1536, 1536], P(None, None, 'shard')
The draws below stay inside these ranges and needn't reach their ends.
Inputs may be any that keep to these rules, and one draw needn't show every extreme that they name: A permutation: block b belongs to the group of replicas b' * (2) to (b' + 1) * 2 - 1 with b' = owner[b]. `inverse_roots`: each matrix has positive diagonal entries.
All inputs are finite; a program needn't handle non-finite values.
Results may differ from the reference program's by a relative error of at most 0.0049.
Values may be sent and summed in bfloat16 or wider, within the bound.
A program may use at most 128 MiB of HBM per device.

```python
import math
import jax
import jax.numpy as jnp
from jax import lax

D = 1536
BLOCKS = 4
TOKENS = 8192


def draw_inverse_roots(key, part):
    base_key = jax.random.fold_in(key, 11)
    key_noise, key_diagonal = jax.random.split(base_key, 2)
    scatter_noise = jax.random.normal(key_noise, (BLOCKS * D, 2, D), jnp.float32) * (0.5 / math.sqrt(D))
    diagonal = jax.random.uniform(key_diagonal, (BLOCKS * D, 2, 1), jnp.float32, 0.5, 1.5)
    within_rows = (jnp.arange(BLOCKS * D, dtype=jnp.int32) % D)[:, None, None]
    column_ids = jnp.arange(D, dtype=jnp.int32)[None, None, :]
    return (scatter_noise + jnp.where(within_rows == column_ids, diagonal, 0.0)).astype(jnp.bfloat16)


def steps_of(stream_key, extent, cuts, low, largest):
    def one(position, shards_of):
        heights = jax.random.uniform(jax.random.fold_in(jax.random.fold_in(stream_key, 6), position), (shards_of,), jnp.float32, low / len(cuts), largest / len(cuts))
        return jnp.repeat(jnp.exp(heights), extent[position] // shards_of).reshape((-1,) + (1,) * (len(extent) - position - 1))

    loudness = one(*cuts[0])
    for cut in cuts[1:]:
        loudness = loudness * one(*cut)
    return loudness


def centred(own_key, dims, deviation, limit, shards=(), kind=jnp.bfloat16):
    values = jax.random.normal(own_key, dims, jnp.float32) * deviation
    if len(shards) > 0:
        values = steps_of(own_key, dims, shards, -0.22, 0.18) * values
    return jnp.clip(values, min=-limit, max=limit).astype(kind)


def setup_inputs(seed: int = 0) -> dict:
    splits = jax.random.split(jax.random.key(seed), 9)
    return {
        "activations": centred(splits[0], (TOKENS, D), 1.0, 6.0, ((0, 8),)),
        "output_grads": centred(splits[1], (TOKENS, BLOCKS, D), (TOKENS * 40) ** -0.5, 0.009765625, ((0, 8), (2, 4))),
        "owner": jax.random.permutation(splits[2], BLOCKS).astype(jnp.int32),
        "step_count": jax.random.randint(splits[3], (1,), 1, 41).astype(jnp.int32),
        "statistics": centred(splits[4], (BLOCKS * D, 2, D), 1.0, 6.0, ((0, 32),), jnp.float32),
        "inverse_roots": draw_inverse_roots(jax.random.fold_in(splits[8], 71), 0),
        "first_moment": centred(splits[6], (BLOCKS * D, D), 0.1, 0.6, ((0, 32),), jnp.float32),
        "second_moment": jnp.clip(jnp.exp(math.log(0.05) - 2.3025851 * jax.random.uniform(splits[7], (BLOCKS * D, D), jnp.float32) ** steps_of(splits[7], (BLOCKS * D, D), ((0, 32),), -0.2, 0.2)), 0.005, 0.05),
    }


beta_stat = 0.9
beta_first = 0.9
beta_second = 0.999
eps_adam = 1e-08
eps_norm = 1e-06

def reference(activations, output_grads, owner, step_count, statistics, inverse_roots, first_moment, second_moment):
    blocks_count = output_grads.shape[1]
    model_width = activations.shape[1]
    slot_ids = jnp.arange(blocks_count, dtype=jnp.int32)
    onehot = (owner[None, :] == slot_ids[:, None]).astype(jnp.int32)
    source = lax.optimization_barrier(jnp.sum(onehot * slot_ids[None, :], axis=1)).astype(jnp.int32)

    def block_grad(block_index):
        douts = lax.dynamic_index_in_dim(output_grads, block_index, 1, keepdims=False)
        return lax.dot_general(activations, douts, (((0,), (0,)), ((), ())), preferred_element_type=jnp.float32)
    exact = lax.map(block_grad, source)
    rounded = exact.astype(jnp.bfloat16)
    stats_slot = statistics.reshape(blocks_count, model_width, 2, model_width)
    roots_slot = inverse_roots.reshape(blocks_count, model_width, 2, model_width)

    def precondition(operands):
        grad_block, stat_block, root_block = operands
        left_gram = lax.dot_general(grad_block, grad_block, (((1,), (1,)), ((), ())), preferred_element_type=jnp.float32)
        right_gram = lax.dot_general(grad_block, grad_block, (((0,), (0,)), ((), ())), preferred_element_type=jnp.float32)
        new_left = beta_stat * stat_block[:, 0, :] + (1.0 - beta_stat) * left_gram
        new_right = beta_stat * stat_block[:, 1, :] + (1.0 - beta_stat) * right_gram
        right_part = lax.dot_general(grad_block, root_block[:, 1, :], (((1,), (1,)), ((), ())), preferred_element_type=jnp.float32)
        precond = jnp.dot(root_block[:, 0, :].astype(jnp.float32), right_part, precision=lax.Precision.HIGHEST)
        return (jnp.stack([new_left, new_right], axis=1), precond)
    new_stats, precond = lax.map(precondition, (rounded, stats_slot, roots_slot))
    flat_grad = exact.reshape(blocks_count * model_width, model_width)
    count_float = step_count[0].astype(jnp.float32)
    first_new = beta_first * first_moment + (1.0 - beta_first) * flat_grad
    second_new = beta_second * second_moment + (1.0 - beta_second) * flat_grad * flat_grad
    first_hat = first_new / (1.0 - jnp.power(beta_first, count_float))
    second_hat = second_new / (1.0 - jnp.power(beta_second, count_float))
    adam_dir = first_hat / (jnp.sqrt(second_hat) + eps_adam)
    adam_squares = lax.optimization_barrier(jnp.sum((adam_dir * adam_dir).reshape(blocks_count, -1), axis=1))
    precond_squares = lax.optimization_barrier(jnp.sum((precond * precond).reshape(blocks_count, -1), axis=1))
    scale = jnp.sqrt(adam_squares) / (jnp.sqrt(precond_squares) + eps_norm)
    grafted = (precond * scale[:, None, None]).astype(jnp.bfloat16)
    update = jnp.take(grafted, owner, axis=0)
    return (new_stats.reshape(blocks_count * model_width, 2, model_width), first_new, second_new, update)
```

```python
import jax
import jax.numpy as jnp
import numpy as np
from jax import lax
from jax.sharding import PartitionSpec as P

beta_stat = 0.9
beta_first = 0.9
beta_second = 0.999
eps_adam = 1e-08
eps_norm = 1e-06


def bits_of(extent):
    return extent.bit_length() - 1


def swap(value, axis, bit, keep=lambda i: True):
    n = lax.axis_size(axis)
    return lax.ppermute(value, axis, [(i, i ^ (1 << bit)) for i in range(n) if keep(i)])


def join(value, partner, axis, bit, dim):
    upper = (lax.axis_index(axis) >> bit) & 1 == 1
    return jnp.where(
        upper,
        jnp.concatenate([partner, value], dim),
        jnp.concatenate([value, partner], dim),
    )


def double(value, axis, bit, dim, keep=lambda i: True):
    return join(value, swap(value, axis, bit, keep), axis, bit, dim)


def reversed_bits(count):
    bits = bits_of(count)
    return [int(format(i, "b").zfill(bits)[::-1], 2) if bits else 0 for i in range(count)]


def reorder(value, count, dim):
    size = value.shape[dim] // count
    return jnp.concatenate(
        [lax.slice_in_dim(value, k * size, (k + 1) * size, axis=dim) for k in reversed_bits(count)],
        dim,
    )


def choose(values, picks, slot):
    out = values[picks[max(picks)]]
    for z in sorted(picks):
        if values[picks[z]] is not out:
            out = jnp.where(slot == z, values[picks[z]], out)
    return out


def body(
    activations,
    output_grads,
    owner,
    step_count,
    statistics,
    inverse_roots,
    first_moment,
    second_moment,
):
    f32, bf16 = jnp.float32, jnp.bfloat16
    width = activations.shape[1]
    groups = output_grads.shape[1]
    replicas = lax.axis_size("replica")
    shards = lax.axis_size("shard")
    size = replicas // groups
    local_bits = range(bits_of(size))
    shard_bits = list(range(bits_of(shards)))[::-1]
    span = statistics.shape[0]
    replica = lax.axis_index("replica")
    slot, local = replica // size, replica % size
    shard = lax.axis_index("shard")
    span_index = local * shards + shard

    slot_ids = jnp.arange(groups, dtype=jnp.int32)
    onehot = (owner[None, :] == slot_ids[:, None]).astype(jnp.int32)
    source = jnp.sum(onehot * slot_ids[None, :], axis=1)

    order = [sorted(range(groups), key=lambda s: (-abs(s - z), s)) for z in range(groups)]
    block_order = jnp.take(source, jnp.take(jnp.asarray(np.array(order, np.int32)), slot, axis=0))
    douts = output_grads.transpose(1, 0, 2)
    rounds = []
    for k in range(groups):
        part = lax.dot_general(
            activations,
            lax.dynamic_index_in_dim(douts, block_order[k], 0, keepdims=False),
            (((0,), (0,)), ((), ())),
            preferred_element_type=f32,
        )
        for bit in list(local_bits)[::-1]:
            half = part.shape[0] // 2
            mine = (local >> bit) & 1
            away = lax.dynamic_slice_in_dim(part, (1 - mine) * half, half, 0).astype(bf16)
            part = lax.dynamic_slice_in_dim(part, mine * half, half, 0) + swap(
                away, "replica", bit
            ).astype(f32)
        rounds.append(part)

    def shift(value, up, senders):
        step = size if up else -size
        return lax.ppermute(
            value,
            "replica",
            [(r, r + step) for r in range(replicas) if r // size in senders],
        )

    came_up = came_down = None
    for t in range(1, groups):
        ups = {z: order[z].index(groups - t + z) for z in range(t)}
        downs = {z: order[z].index(z + t - groups) for z in range(groups - t, groups)}
        up = choose(rounds, ups, slot)
        down = choose(rounds, downs, slot)
        if came_up is not None:
            up = up + came_up.astype(f32)
            down = down + came_down.astype(f32)
        came_up = shift(up.astype(bf16), True, ups)
        came_down = shift(down.astype(bf16), False, downs)
    own = (rounds[-1] + came_up.astype(f32) + came_down.astype(f32)).astype(bf16)

    rows = own.shape[0]
    top, low = own[: rows // 2], own[rows // 2 :]
    for bit in local_bits:
        top = double(top, "replica", bit, 0)
    for bit in shard_bits[:-1]:
        low = double(low, "shard", bit, 1)
        top = double(top, "shard", bit, 1)
    for bit in local_bits:
        low = double(low, "replica", bit, 0)
    for bit in shard_bits[-1:]:
        low = double(low, "shard", bit, 1)
        top = double(top, "shard", bit, 1)
    pieces = []
    for k in range(size):
        for half in (top, low):
            pieces.append(lax.slice_in_dim(half, k * (rows // 2), (k + 1) * (rows // 2), axis=0))
    full_grad = reorder(jnp.concatenate(pieces, 0), shards, 1)

    left_root = inverse_roots[:, 0, :]
    for bit in shard_bits:
        left_root = double(left_root, "shard", bit, 0)
    left_root = reorder(left_root, shards, 0)
    pairs = []
    for r in range(replicas):
        for s in range(shards):
            j = (r % size) * shards + s
            target = (r // size * size + j % size) * shards + j // size
            pairs.append((r * shards + s, target))
    right_root = lax.ppermute(inverse_roots[:, 1, :], ("replica", "shard"), pairs)
    for bit in local_bits:
        right_root = double(right_root, "replica", bit, 0)

    right_part = lax.dot_general(
        full_grad, right_root, (((1,), (1,)), ((), ())), preferred_element_type=f32
    )
    high = lax.reduce_precision(right_part, 8, 7)
    rest = right_part - high
    precond = jnp.dot(left_root, high.astype(bf16), preferred_element_type=f32) + jnp.dot(
        left_root, rest.astype(bf16), preferred_element_type=f32
    )

    rounded = lax.dynamic_slice_in_dim(full_grad, span_index * span, span, 0)
    exact = rounded.astype(f32)
    count_float = step_count[0].astype(f32)
    first_new = beta_first * first_moment + (1.0 - beta_first) * exact
    second_new = beta_second * second_moment + (1.0 - beta_second) * exact * exact
    first_hat = first_new / (1.0 - jnp.power(beta_first, count_float))
    second_hat = second_new / (1.0 - jnp.power(beta_second, count_float))
    adam_dir = first_hat / (jnp.sqrt(second_hat) + eps_adam)

    sums = jnp.stack([jnp.sum(adam_dir * adam_dir), jnp.sum(precond * precond)])
    sums = jnp.broadcast_to(sums[:, None], (2, 128))
    for bit in local_bits:
        sums = sums + swap(sums, "replica", bit)
    for bit in shard_bits:
        sums = sums + swap(sums, "shard", bit)
    scale = jnp.sqrt(sums[0, 0]) / (jnp.sqrt(sums[1, 0]) + eps_norm)
    grafted = (precond * scale).astype(bf16)

    def complete(value, zs):
        for bit in local_bits:
            value = double(value, "replica", bit, 0, lambda r: r // size in zs)
        return value

    whole = {0: complete(grafted, range(groups))}
    up = down = grafted
    ups, downs = {}, {}
    for t in range(1, groups):
        up = shift(up, True, range(t - 1, groups - 1))
        down = shift(down, False, range(1, groups - t + 1))
        ups[t] = complete(up, range(t, groups))
        downs[t] = complete(down, range(0, groups - t))
    for m in range(1, groups):
        whole[m] = jnp.where(slot + m < groups, downs[m], ups[groups - m])
    update = jnp.zeros((groups,) + whole[0].shape, bf16)
    for m in range(groups):
        block = jnp.take(source, (slot + m) % groups)
        update = lax.dynamic_update_index_in_dim(update, whole[m], block, 0)

    grad_columns = lax.dynamic_slice_in_dim(full_grad, span_index * span, span, 1)
    left_gram = lax.dot_general(
        rounded, full_grad, (((1,), (1,)), ((), ())), preferred_element_type=f32
    )
    right_gram = lax.dot_general(
        grad_columns, full_grad, (((0,), (0,)), ((), ())), preferred_element_type=f32
    )
    new_left = beta_stat * statistics[:, 0, :] + (1.0 - beta_stat) * left_gram
    new_right = beta_stat * statistics[:, 1, :] + (1.0 - beta_stat) * right_gram
    new_stats = jnp.stack([new_left, new_right], axis=1)
    return (new_stats, first_new, second_new, update)


def solution(mesh):
    placed = (
        P("replica", None),
        P("replica", None, "shard"),
        P(),
        P(),
        P(("replica", "shard"), None, None),
        P(("replica", "shard"), None, None),
        P(("replica", "shard"), None),
        P(("replica", "shard"), None),
    )
    return jax.shard_map(
        body,
        mesh=mesh,
        in_specs=placed,
        out_specs=(
            P(("replica", "shard"), None, None),
            P(("replica", "shard"), None),
            P(("replica", "shard"), None),
            P(None, None, "shard"),
        ),
        check_vma=False,
    )
```
